256 devices in a mesh: groups: 4 (over y, x), dp: 64 (over z, core).
Axes of the slice: x: 2, y: 2, z: 32, core: 2. Of those that a mesh axis runs over, the one named last changes fastest.
The devices are a block of a 4x8x32 slice.
Arguments:
- inputs: bfloat16 [2048, 32, 8192], P(('groups', 'dp')), parts along dimension 0, may hold values from -6 to 6
- out_grads: bfloat16 [2048, 32, 8192], P(('groups', 'dp')), parts along dimension 0, may hold values from -3 to 3
- token_ids: int32 [2048, 32], P(('groups', 'dp')), parts along dimension 0, may hold values from 0 to 128255
- in_signs: int32 [64, 8192], replicated, may hold values from 0 to 1
- out_signs: int32 [64, 8192], replicated, may hold values from 0 to 1
Outputs:
- fisher_block: bfloat16 [16384, 4096], P(('groups', 'dp')), parts along dimension 0
- precond_features: float32 [2048, 4096], P(('groups', 'dp')), parts along dimension 0
The draws below stay inside these ranges and needn't reach their ends.
There are 4 independent parts, one for each index of `groups`. The reference program is written for one: setup_inputs(seed, part) draws one part's arguments, and reference() takes and returns one part's arrays. A program takes and returns all parts, laid end to end along the dimension named above; an argument that names none is the same for every part. Nothing has to cross between parts.
All inputs are finite; a program needn't handle non-finite values.
Results may differ from the reference program's by a relative error of at most 0.0057.
Values may be sent and summed in bfloat16 or wider, within the bound.
No kernel may reach another device: no remote copies, remote signals or barrier semaphores. Data moves between devices by JAX's collectives and lax.ppermute only.
A program may use at most 64 MiB of HBM per device.

```python
import math
import jax
import jax.numpy as jnp
from jax import lax

D = 8192
OUT = 8192
VOCAB = 128256
KP = 64
LEN = 32
RESERVED = 32064
NSAMP = 512


def draw_out_grads(key, part):
    noise_key = jax.random.fold_in(key, 11)
    spread_key = jax.random.fold_in(key, 12)
    place = jnp.arange(NSAMP, dtype=jnp.float32) / max(NSAMP - 1, 1)
    rising = jnp.sqrt(1.0 + 2.0 * place)
    spread = jnp.exp(jax.random.uniform(spread_key, (NSAMP,), jnp.float32, 0.0, 0.5 * math.log(10.0)))
    row_scale = 0.5 * LEN ** (-0.5) * rising * spread
    noise = jax.random.normal(noise_key, (NSAMP, LEN, OUT), jnp.float32)
    values = noise * row_scale[:, None, None]
    return jnp.clip(values, -3.0, 3.0).astype(jnp.bfloat16)


def place_ends(values, rng, low, high):
    spot = [jax.random.randint(jax.random.fold_in(rng, axis), (), 0, length) for axis, length in enumerate(values.shape)]
    longest = values.shape.index(max(values.shape))
    beside = spot[:longest] + [(spot[longest] + 1) % values.shape[longest]] + spot[longest + 1:]
    return values.at[tuple(spot)].set(low).at[tuple(beside)].set(high)


def block_scale(key, dims, split, low, high):
    factor_of = 1.0
    for position, shards_of in split:
        draws = jax.random.uniform(jax.random.fold_in(jax.random.fold_in(key, 6), position), (shards_of,), jnp.float32, low / len(split), high / len(split))
        factor_of = factor_of * jnp.repeat(jnp.exp(draws), dims[position] // shards_of).reshape((-1,) + (1,) * (len(dims) - 1 - position))
    return factor_of


def normal_values(rng, extent, deviation, most, split=(), kind=jnp.bfloat16):
    values = deviation * jax.random.normal(rng, extent, jnp.float32)
    if split:
        values = values * block_scale(rng, extent, split, -0.22, 0.18)
    return jnp.clip(values, -most, most).astype(kind)


def setup_inputs(seed: int = 0, part: int = 0) -> dict:
    splits = jax.random.split(jax.random.key(seed), 6)
    part_keys = jax.random.split(jax.random.fold_in(splits[5], part), 6)
    inputs = normal_values(part_keys[0], (NSAMP, LEN, D), 1.0, 6.0, ((0, 64),))
    out_grads = draw_out_grads(jax.random.fold_in(jax.random.fold_in(splits[5], part), 71), part)
    token_ids = place_ends(jax.random.randint(part_keys[2], (NSAMP, LEN), 0, VOCAB), jax.random.fold_in(part_keys[2], 1), 0, VOCAB - 1).astype(jnp.int32)
    in_signs = place_ends(jax.random.randint(splits[3], (KP, D), 0, 2), jax.random.fold_in(splits[3], 1), 0, 1).astype(jnp.int32)
    out_signs = place_ends(jax.random.randint(splits[4], (KP, OUT), 0, 2), jax.random.fold_in(splits[4], 1), 0, 1).astype(jnp.int32)
    return dict(inputs=inputs, out_grads=out_grads, token_ids=token_ids, in_signs=in_signs, out_signs=out_signs)


def project(values, sign_bits):
    sign_table = 2.0 * sign_bits.astype(jnp.float32) - 1.0
    in_width = values.shape[-1]

    def project_one(sequence):
        rows_wide = sequence.astype(jnp.float32)
        return jnp.dot(rows_wide, sign_table.T, precision=lax.Precision.HIGHEST) * in_width ** (-0.5)
    return lax.map(project_one, values)

def reference(inputs, out_grads, token_ids, in_signs, out_signs):
    keep_mask = (token_ids >= RESERVED).astype(jnp.float32)
    in_proj = project(inputs, in_signs) * keep_mask[:, :, None]
    out_proj = project(out_grads, out_signs)
    outer = jnp.einsum('sti,stj->sij', in_proj, out_proj, precision=lax.Precision.HIGHEST)
    per_sample = outer.reshape(outer.shape[0], -1).astype(jnp.bfloat16)
    samples = per_sample.shape[0]
    features = per_sample.shape[1]
    fisher = jnp.dot(per_sample.T.astype(jnp.float32), per_sample.astype(jnp.float32), preferred_element_type=jnp.float32) / samples
    damping = jnp.trace(fisher) / features
    system = fisher + damping * jnp.eye(features, dtype=jnp.float32)
    grads_wide = per_sample.astype(jnp.float32)
    precond_features = damping * jnp.linalg.solve(system, grads_wide.T).T
    return (fisher.astype(jnp.bfloat16), precond_features)
```

```python
import functools

import jax
import jax.numpy as jnp
from jax import lax
from jax.experimental import pallas as pl
from jax.experimental.pallas import tpu as pltpu
from jax.sharding import PartitionSpec as P

RESERVED = 32064
TOLERANCE = 1e-5


def project(values, sign_bits):
    sign_table = (2 * sign_bits - 1).astype(jnp.bfloat16)
    in_width = values.shape[-1]
    flat_rows = values.reshape(-1, in_width)
    product = lax.dot_general(
        flat_rows, sign_table, (((1,), (1,)), ((), ())), preferred_element_type=jnp.float32
    )
    return product * in_width ** (-0.5)


def gather_samples(own, axis):
    chips = lax.axis_size(axis) // 2
    turn = [(2 * z + c, 2 * z + 1 - c) for z in range(chips) for c in range(2)]

    def along(value, hops):
        pairs = [(2 * z, 2 * ((z + hops) % chips)) for z in range(chips)]
        pairs += [(2 * z + 1, 2 * ((z - hops) % chips) + 1) for z in range(chips)]
        return lax.ppermute(value, axis, pairs)

    carried = [own, lax.ppermute(own, axis, turn)]
    held = [own]
    far = chips // 2
    for distance in range(0, far, 2):
        last = distance + 2 == far
        onward = [along(value, 2) for value in (carried[:1] if last else carried)]
        held += [along(value, 1) for value in carried]
        held += onward
        carried = onward
    half = jnp.concatenate(held, axis=0)
    return jnp.concatenate([half, lax.ppermute(half, axis, turn)], axis=0)


def split3(value):
    high = value.astype(jnp.bfloat16)
    rest = value - high.astype(jnp.float32)
    mid = rest.astype(jnp.bfloat16)
    low = (rest - mid.astype(jnp.float32)).astype(jnp.bfloat16)
    return high, mid, low


def stack3(value):
    parts = [part.astype(jnp.float32) for part in split3(value)]
    return jnp.concatenate([*parts, jnp.zeros_like(value)], axis=0).astype(jnp.bfloat16)


def dot(left, right, dims=(1, 0)):
    return lax.dot_general(
        left, right, (((dims[0],), (dims[1],)), ((), ())), preferred_element_type=jnp.float32
    )


def tail_kernel(place_ref, all_ref, fisher_ref, precond_ref, columns_ref, high_ref, mid_ref, low_ref):
    samples, features = all_ref.shape
    own_rows = fisher_ref.shape[0]
    count = precond_ref.shape[0]
    gram = dot(all_ref[...], all_ref[...], (1, 1))
    row = lax.broadcasted_iota(jnp.int32, gram.shape, 0)
    column = lax.broadcasted_iota(jnp.int32, gram.shape, 1)
    on_diagonal = row == column
    diagonal = jnp.where(on_diagonal, gram, 0.0)
    across = jnp.sum(diagonal, axis=0, keepdims=True)
    down = jnp.sum(diagonal, axis=1, keepdims=True)
    factor = features / jnp.sum(across)
    across = lax.rsqrt(1.0 + factor * across)
    down = lax.rsqrt(1.0 + factor * down)
    system = (jnp.where(on_diagonal, 1.0, 0.0) + factor * gram) * (down * across)
    high_ref[...], mid_ref[...], low_ref[...] = split3(system)

    def apply(rows):
        stacked = stack3(rows)
        by_high = dot(stacked, high_ref[...])
        by_mid = dot(stacked[: 2 * count], mid_ref[...])
        by_low = dot(stacked[: 2 * count], low_ref[...])
        small = by_low[:count] + by_mid[count:] + by_high[2 * count : 3 * count]
        return by_high[:count] + (by_mid[:count] + by_high[count : 2 * count] + small)

    unit_row = lax.broadcasted_iota(jnp.int32, (count, samples), 0)
    unit_column = lax.broadcasted_iota(jnp.int32, (count, samples), 1)
    right = jnp.where(unit_row == unit_column, across, 0.0)
    start = jnp.sum(right * right, axis=1, keepdims=True)
    limit = TOLERANCE * TOLERANCE * start

    def step(solved, residual, direction, squares):
        image = apply(direction)
        curvature = jnp.sum(direction * image, axis=1, keepdims=True)
        length = squares / jnp.maximum(curvature, 1e-37)
        solved = solved + length * direction
        residual = residual - length * image
        new_squares = jnp.sum(residual * residual, axis=1, keepdims=True)
        direction = residual + (new_squares / jnp.maximum(squares, 1e-37)) * direction
        return solved, residual, direction, new_squares

    def unfinished(carry):
        index, open_rows, *_ = carry
        return jnp.logical_and(index < 4 * samples, open_rows > 0.0)

    def body(carry):
        index, _, *state = carry
        for _ in range(2):
            state = step(*state)
        open_rows = jnp.max(jnp.where(state[3] > limit, 1.0, 0.0))
        return (index + 2, open_rows, *state)

    first = (jnp.int32(0), jnp.float32(1.0), jnp.zeros_like(right), right, right, start)
    solved = lax.while_loop(unfinished, body, first)[2]

    place = place_ref[0]
    lanes = columns_ref.shape[0]
    block = pl.multiple_of((place * own_rows // lanes) * lanes, lanes)
    columns_ref[...] = all_ref[:, pl.ds(block, lanes)].astype(jnp.float32).T
    inside = pl.multiple_of(place * own_rows % lanes, own_rows)
    columns = columns_ref[pl.ds(inside, own_rows), :].astype(jnp.bfloat16)
    both = dot(jnp.concatenate([columns, stack3(solved * across)], axis=0), all_ref[...])
    fisher_ref[...] = (both[:own_rows] * (1.0 / samples)).astype(jnp.bfloat16)
    low, mid, high = (both[own_rows + k * count : own_rows + (k + 1) * count] for k in (2, 1, 0))
    precond_ref[...] = high + (mid + low)


def tail(gathered, place, count, own_rows):
    samples, features = gathered.shape
    vmem = pl.BlockSpec(memory_space=pltpu.VMEM)
    return pl.pallas_call(
        tail_kernel,
        name="fisher_and_solve",
        out_shape=(
            jax.ShapeDtypeStruct((own_rows, features), jnp.bfloat16),
            jax.ShapeDtypeStruct((count, features), jnp.float32),
        ),
        in_specs=[pl.BlockSpec(memory_space=pltpu.SMEM), vmem],
        out_specs=(vmem, vmem),
        scratch_shapes=[
            pltpu.VMEM((128, samples), jnp.float32),
            *[pltpu.VMEM((samples, samples), jnp.bfloat16)] * 3,
        ],
    )(place, gathered)


def on_device(inputs, out_grads, token_ids, in_signs, out_signs):
    local_count, length = token_ids.shape
    keep_mask = (token_ids >= RESERVED).astype(jnp.float32).reshape(-1, 1)
    in_proj = (project(inputs, in_signs) * keep_mask).reshape(local_count, length, -1)
    out_proj = project(out_grads, out_signs).reshape(local_count, length, -1)
    outer = jnp.einsum("sti,stj->sij", in_proj, out_proj, precision=lax.Precision.HIGHEST)
    per_sample = outer.reshape(local_count, -1).astype(jnp.bfloat16)
    gathered = gather_samples(per_sample, "dp")
    own_rows = per_sample.shape[1] // lax.axis_size("dp")
    place = lax.axis_index("dp").astype(jnp.int32).reshape(1)
    return tail(gathered, place, local_count, own_rows)


def solution(mesh):
    in_specs = (
        P(("groups", "dp"), None, None),
        P(("groups", "dp"), None, None),
        P(("groups", "dp"), None),
        P(),
        P(),
    )
    out_specs = (P(("groups", "dp"), None), P(("groups", "dp"), None))
    return jax.shard_map(
        on_device, mesh=mesh, in_specs=in_specs, out_specs=out_specs, check_vma=False
    )
```

```python
import functools

import jax
import jax.numpy as jnp
from jax import lax
from jax.experimental import pallas as pl
from jax.experimental.pallas import tpu as pltpu
from jax.sharding import PartitionSpec as P

RESERVED = 32064
TOLERANCE = 1e-5
KERNEL_VMEM = 24 * 2**20


def project(values, sign_bits):
    sign_table = (2 * sign_bits - 1).astype(jnp.bfloat16)
    in_width = values.shape[-1]
    flat_rows = values.reshape(-1, in_width)
    product = lax.dot_general(
        flat_rows, sign_table, (((1,), (1,)), ((), ())), preferred_element_type=jnp.float32
    )
    return product * in_width ** (-0.5)


def gather_samples(own, axis):
    chips = lax.axis_size(axis) // 2
    turn = [(2 * z + c, 2 * z + 1 - c) for z in range(chips) for c in range(2)]

    def along(value, hops):
        pairs = [(2 * z, 2 * ((z + hops) % chips)) for z in range(chips)]
        pairs += [(2 * z + 1, 2 * ((z - hops) % chips) + 1) for z in range(chips)]
        return lax.ppermute(value, axis, pairs)

    carried = [own, lax.ppermute(own, axis, turn)]
    held = [own]
    far = chips // 2
    for distance in range(0, far, 2):
        last = distance + 2 == far
        onward = [along(value, 2) for value in (carried[:1] if last else carried)]
        held += [along(value, 1) for value in carried]
        held += onward
        carried = onward
    cuts = (0, chips // 2, 3 * chips // 4, chips)
    halves = [jnp.concatenate(held[low:high], axis=0) for low, high in zip(cuts, cuts[1:])]
    blocks = [block for half in halves for block in (half, lax.ppermute(half, axis, turn))]
    return blocks[:-2], blocks[-2:]


def split3(value):
    high = value.astype(jnp.bfloat16)
    rest = value - high.astype(jnp.float32)
    mid = rest.astype(jnp.bfloat16)
    low = (rest - mid.astype(jnp.float32)).astype(jnp.bfloat16)
    return high, mid, low


def stack3(value):
    parts = [part.astype(jnp.float32) for part in split3(value)]
    return jnp.concatenate([*parts, jnp.zeros_like(value)], axis=0).astype(jnp.bfloat16)


def dot(left, right, dims=(1, 0)):
    return lax.dot_general(
        left, right, (((dims[0],), (dims[1],)), ((), ())), preferred_element_type=jnp.float32
    )


def join(blocks, out_ref):
    start = 0
    for block in blocks:
        out_ref[start : start + block.shape[0]] = block[...]
        start += block.shape[0]


def early_kernel(*refs):
    *blocks, rows_ref, gram_ref = refs
    join(blocks, rows_ref)
    gram_ref[...] = dot(rows_ref[...], rows_ref[...], (1, 1))


def early(blocks):
    count, features = sum(block.shape[0] for block in blocks), blocks[0].shape[1]
    vmem = pl.BlockSpec(memory_space=pltpu.VMEM)
    return pl.pallas_call(
        early_kernel,
        name="early_gram",
        out_shape=(
            jax.ShapeDtypeStruct((count, features), jnp.bfloat16),
            jax.ShapeDtypeStruct((count, count), jnp.float32),
        ),
        in_specs=[vmem] * len(blocks),
        out_specs=(vmem, vmem),
        cost_estimate=pl.CostEstimate(
            flops=2 * count * count * features, bytes_accessed=4 * count * features, transcendentals=0
        ),
        compiler_params=pltpu.CompilerParams(vmem_limit_bytes=KERNEL_VMEM),
    )(*blocks)


def tail_kernel(place_ref, first_ref, first_gram_ref, *refs):
    *blocks, fisher_ref, precond_ref, columns_ref, high_ref, mid_ref, low_ref, late_ref, gram_ref = refs
    earlier, features = first_ref.shape
    samples = gram_ref.shape[0]
    own_rows = fisher_ref.shape[0]
    count = precond_ref.shape[0]
    join(blocks, late_ref)
    late_gram = dot(late_ref[...], first_ref[...], (1, 1))
    gram_ref[:earlier, :earlier] = first_gram_ref[...]
    gram_ref[earlier:, :earlier] = late_gram
    gram_ref[:earlier, earlier:] = late_gram.T
    gram_ref[earlier:, earlier:] = dot(late_ref[...], late_ref[...], (1, 1))
    gram = gram_ref[...]
    row = lax.broadcasted_iota(jnp.int32, gram.shape, 0)
    column = lax.broadcasted_iota(jnp.int32, gram.shape, 1)
    on_diagonal = row == column
    diagonal = jnp.where(on_diagonal, gram, 0.0)
    across = jnp.sum(diagonal, axis=0, keepdims=True)
    down = jnp.sum(diagonal, axis=1, keepdims=True)
    factor = features / jnp.sum(across)
    across = lax.rsqrt(1.0 + factor * across)
    down = lax.rsqrt(1.0 + factor * down)
    system = (jnp.where(on_diagonal, 1.0, 0.0) + factor * gram) * (down * across)
    high_ref[...], mid_ref[...], low_ref[...] = split3(system)

    def apply(rows):
        stacked = stack3(rows)
        by_high = dot(stacked, high_ref[...])
        by_mid = dot(stacked[: 2 * count], mid_ref[...])
        by_low = dot(stacked[: 2 * count], low_ref[...])
        small = by_low[:count] + by_mid[count:] + by_high[2 * count : 3 * count]
        return by_high[:count] + (by_mid[:count] + by_high[count : 2 * count] + small)

    unit_row = lax.broadcasted_iota(jnp.int32, (count, samples), 0)
    unit_column = lax.broadcasted_iota(jnp.int32, (count, samples), 1)
    right = jnp.where(unit_row == unit_column, across, 0.0)
    start = jnp.sum(right * right, axis=1, keepdims=True)
    limit = TOLERANCE * TOLERANCE * start

    def step(solved, residual, direction, squares):
        image = apply(direction)
        curvature = jnp.sum(direction * image, axis=1, keepdims=True)
        length = squares / jnp.maximum(curvature, 1e-37)
        solved = solved + length * direction
        residual = residual - length * image
        new_squares = jnp.sum(residual * residual, axis=1, keepdims=True)
        direction = residual + (new_squares / jnp.maximum(squares, 1e-37)) * direction
        return solved, residual, direction, new_squares

    def unfinished(carry):
        index, open_rows, *_ = carry
        return jnp.logical_and(index < 4 * samples, open_rows > 0.0)

    def body(carry):
        index, _, *state = carry
        for _ in range(2):
            state = step(*state)
        open_rows = jnp.max(jnp.where(state[3] > limit, 1.0, 0.0))
        return (index + 2, open_rows, *state)

    first = (jnp.int32(0), jnp.float32(1.0), jnp.zeros_like(right), right, right, start)
    solved = lax.while_loop(unfinished, body, first)[2]

    place = place_ref[0]
    lanes = columns_ref.shape[0]
    block = pl.multiple_of((place * own_rows // lanes) * lanes, lanes)
    columns_ref[:, :earlier] = first_ref[:, pl.ds(block, lanes)].astype(jnp.float32).T
    columns_ref[:, earlier:] = late_ref[:, pl.ds(block, lanes)].astype(jnp.float32).T
    inside = pl.multiple_of(place * own_rows % lanes, own_rows)
    columns = columns_ref[pl.ds(inside, own_rows), :].astype(jnp.bfloat16)
    left = jnp.concatenate([columns, stack3(solved * across)], axis=0)
    both = dot(left[:, :earlier], first_ref[...]) + dot(left[:, earlier:], late_ref[...])
    fisher_ref[...] = (both[:own_rows] * (1.0 / samples)).astype(jnp.bfloat16)
    low, mid, high = (both[own_rows + k * count : own_rows + (k + 1) * count] for k in (2, 1, 0))
    precond_ref[...] = high + (mid + low)


def tail(place, rows, gram, blocks, count, own_rows):
    late, features = sum(block.shape[0] for block in blocks), rows.shape[1]
    samples = rows.shape[0] + late
    vmem = pl.BlockSpec(memory_space=pltpu.VMEM)
    return pl.pallas_call(
        tail_kernel,
        name="fisher_and_solve",
        out_shape=(
            jax.ShapeDtypeStruct((own_rows, features), jnp.bfloat16),
            jax.ShapeDtypeStruct((count, features), jnp.float32),
        ),
        in_specs=[pl.BlockSpec(memory_space=pltpu.SMEM)] + [vmem] * (2 + len(blocks)),
        out_specs=(vmem, vmem),
        scratch_shapes=[
            pltpu.VMEM((128, samples), jnp.float32),
            *[pltpu.VMEM((samples, samples), jnp.bfloat16)] * 3,
            pltpu.VMEM((late, features), jnp.bfloat16),
            pltpu.VMEM((samples, samples), jnp.float32),
        ],
        compiler_params=pltpu.CompilerParams(vmem_limit_bytes=KERNEL_VMEM),
    )(place, rows, gram, *blocks)


def on_device(inputs, out_grads, token_ids, in_signs, out_signs):
    local_count, length = token_ids.shape
    keep_mask = (token_ids >= RESERVED).astype(jnp.float32).reshape(-1, 1)
    in_proj = (project(inputs, in_signs) * keep_mask).reshape(local_count, length, -1)
    out_proj = project(out_grads, out_signs).reshape(local_count, length, -1)
    outer = jnp.einsum("sti,stj->sij", in_proj, out_proj, precision=lax.Precision.HIGHEST)
    per_sample = outer.reshape(local_count, -1).astype(jnp.bfloat16)
    first, last = gather_samples(per_sample, "dp")
    rows, gram = early(first)
    own_rows = per_sample.shape[1] // lax.axis_size("dp")
    place = lax.axis_index("dp").astype(jnp.int32).reshape(1)
    return tail(place, rows, gram, last, local_count, own_rows)


def solution(mesh):
    in_specs = (
        P(("groups", "dp"), None, None),
        P(("groups", "dp"), None, None),
        P(("groups", "dp"), None),
        P(),
        P(),
    )
    out_specs = (P(("groups", "dp"), None), P(("groups", "dp"), None))
    return jax.shard_map(
        on_device, mesh=mesh, in_specs=in_specs, out_specs=out_specs, check_vma=False
    )
```

```python
import functools

import jax
import jax.numpy as jnp
from jax import lax
from jax.experimental import pallas as pl
from jax.experimental.pallas import tpu as pltpu
from jax.sharding import PartitionSpec as P

RESERVED = 32064
TOLERANCE = 1e-5
KERNEL_VMEM = 24 * 2**20


def project(values, sign_bits):
    sign_table = (2 * sign_bits - 1).astype(jnp.bfloat16)
    in_width = values.shape[-1]
    flat_rows = values.reshape(-1, in_width)
    product = lax.dot_general(
        flat_rows, sign_table, (((1,), (1,)), ((), ())), preferred_element_type=jnp.float32
    )
    return product * in_width ** (-0.5)


def gather_samples(own, axis):
    chips = lax.axis_size(axis) // 2
    turn = [(2 * z + c, 2 * z + 1 - c) for z in range(chips) for c in range(2)]

    def along(value, hops):
        pairs = [(2 * z, 2 * ((z + hops) % chips)) for z in range(chips)]
        pairs += [(2 * z + 1, 2 * ((z - hops) % chips) + 1) for z in range(chips)]
        return lax.ppermute(value, axis, pairs)

    carried = [own, lax.ppermute(own, axis, turn)]
    held = [own]
    far = chips // 2
    for distance in range(0, far, 2):
        last = distance + 2 == far
        onward = [along(value, 2) for value in (carried[:1] if last else carried)]
        held += [along(jnp.concatenate(carried, axis=0), 1)]
        held += onward
        carried = onward
    cuts = (0, 3 * chips // 8, 9 * chips // 16)
    halves = [jnp.concatenate(held[low:high], axis=0) for low, high in zip(cuts, cuts[1:])]
    blocks = [block for half in halves for block in (half, lax.ppermute(half, axis, turn))]
    return blocks, held[cuts[-1] :], lambda half: (half, lax.ppermute(half, axis, turn))


def split3(value):
    high = value.astype(jnp.bfloat16)
    rest = value - high.astype(jnp.float32)
    mid = rest.astype(jnp.bfloat16)
    low = (rest - mid.astype(jnp.float32)).astype(jnp.bfloat16)
    return high, mid, low


def stack3(value):
    parts = [part.astype(jnp.float32) for part in split3(value)]
    return jnp.concatenate([*parts, jnp.zeros_like(value)], axis=0).astype(jnp.bfloat16)


def dot(left, right, dims=(1, 0)):
    return lax.dot_general(
        left, right, (((dims[0],), (dims[1],)), ((), ())), preferred_element_type=jnp.float32
    )


def join(blocks, out_ref):
    start = 0
    for block in blocks:
        out_ref[start : start + block.shape[0]] = block[...]
        start += block.shape[0]


def early_kernel(*refs):
    *blocks, rows_ref, gram_ref = refs
    join(blocks, rows_ref)
    gram_ref[...] = dot(rows_ref[...], rows_ref[...], (1, 1))


def early(blocks):
    count, features = sum(block.shape[0] for block in blocks), blocks[0].shape[1]
    vmem = pl.BlockSpec(memory_space=pltpu.VMEM)
    return pl.pallas_call(
        early_kernel,
        name="early_gram",
        out_shape=(
            jax.ShapeDtypeStruct((count, features), jnp.bfloat16),
            jax.ShapeDtypeStruct((count, count), jnp.float32),
        ),
        in_specs=[vmem] * len(blocks),
        out_specs=(vmem, vmem),
        cost_estimate=pl.CostEstimate(
            flops=2 * count * count * features, bytes_accessed=4 * count * features, transcendentals=0
        ),
        compiler_params=pltpu.CompilerParams(vmem_limit_bytes=KERNEL_VMEM),
    )(*blocks)


def tail_kernel(place_ref, first_ref, first_gram_ref, *refs):
    *blocks, fisher_ref, precond_ref, columns_ref, high_ref, mid_ref, low_ref, late_ref, gram_ref = refs
    earlier, features = first_ref.shape
    samples = gram_ref.shape[0]
    own_rows = fisher_ref.shape[0]
    count = precond_ref.shape[0]
    join(blocks, late_ref)
    late_gram = dot(late_ref[...], first_ref[...], (1, 1))
    gram_ref[:earlier, :earlier] = first_gram_ref[...]
    gram_ref[earlier:, :earlier] = late_gram
    gram_ref[:earlier, earlier:] = late_gram.T
    gram_ref[earlier:, earlier:] = dot(late_ref[...], late_ref[...], (1, 1))
    gram = gram_ref[...]
    row = lax.broadcasted_iota(jnp.int32, gram.shape, 0)
    column = lax.broadcasted_iota(jnp.int32, gram.shape, 1)
    on_diagonal = row == column
    diagonal = jnp.where(on_diagonal, gram, 0.0)
    across = jnp.sum(diagonal, axis=0, keepdims=True)
    down = jnp.sum(diagonal, axis=1, keepdims=True)
    factor = features / jnp.sum(across)
    across = lax.rsqrt(1.0 + factor * across)
    down = lax.rsqrt(1.0 + factor * down)
    system = (jnp.where(on_diagonal, 1.0, 0.0) + factor * gram) * (down * across)
    high_ref[...], mid_ref[...], low_ref[...] = split3(system)

    def apply(rows):
        stacked = stack3(rows)
        by_high = dot(stacked, high_ref[...])
        by_mid = dot(stacked[: 2 * count], mid_ref[...])
        by_low = dot(stacked[: 2 * count], low_ref[...])
        small = by_low[:count] + by_mid[count:] + by_high[2 * count : 3 * count]
        return by_high[:count] + (by_mid[:count] + by_high[count : 2 * count] + small)

    unit_row = lax.broadcasted_iota(jnp.int32, (count, samples), 0)
    unit_column = lax.broadcasted_iota(jnp.int32, (count, samples), 1)
    right = jnp.where(unit_row == unit_column, across, 0.0)
    start = jnp.sum(right * right, axis=1, keepdims=True)
    limit = TOLERANCE * TOLERANCE * start

    def step(solved, residual, direction, squares):
        image = apply(direction)
        curvature = jnp.sum(direction * image, axis=1, keepdims=True)
        length = squares / jnp.maximum(curvature, 1e-37)
        solved = solved + length * direction
        residual = residual - length * image
        new_squares = jnp.sum(residual * residual, axis=1, keepdims=True)
        direction = residual + (new_squares / jnp.maximum(squares, 1e-37)) * direction
        return solved, residual, direction, new_squares

    def unfinished(carry):
        index, open_rows, *_ = carry
        return jnp.logical_and(index < 4 * samples, open_rows > 0.0)

    def body(carry):
        index, _, *state = carry
        for _ in range(2):
            state = step(*state)
        open_rows = jnp.max(jnp.where(state[3] > limit, 1.0, 0.0))
        return (index + 2, open_rows, *state)

    first = (jnp.int32(0), jnp.float32(1.0), jnp.zeros_like(right), right, right, start)
    solved = lax.while_loop(unfinished, body, first)[2]

    place = place_ref[0]
    lanes = columns_ref.shape[0]
    block = pl.multiple_of((place * own_rows // lanes) * lanes, lanes)
    columns_ref[:, :earlier] = first_ref[:, pl.ds(block, lanes)].astype(jnp.float32).T
    columns_ref[:, earlier:] = late_ref[:, pl.ds(block, lanes)].astype(jnp.float32).T
    inside = pl.multiple_of(place * own_rows % lanes, own_rows)
    columns = columns_ref[pl.ds(inside, own_rows), :].astype(jnp.bfloat16)
    left = jnp.concatenate([columns, stack3(solved * across)], axis=0)
    both = dot(left[:, :earlier], first_ref[...]) + dot(left[:, earlier:], late_ref[...])
    fisher_ref[...] = (both[:own_rows] * (1.0 / samples)).astype(jnp.bfloat16)
    low, mid, high = (both[own_rows + k * count : own_rows + (k + 1) * count] for k in (2, 1, 0))
    precond_ref[...] = high + (mid + low)


def tail(place, rows, gram, blocks, count, own_rows):
    late, features = sum(block.shape[0] for block in blocks), rows.shape[1]
    samples = rows.shape[0] + late
    vmem = pl.BlockSpec(memory_space=pltpu.VMEM)
    return pl.pallas_call(
        tail_kernel,
        name="fisher_and_solve",
        out_shape=(
            jax.ShapeDtypeStruct((own_rows, features), jnp.bfloat16),
            jax.ShapeDtypeStruct((count, features), jnp.float32),
        ),
        in_specs=[pl.BlockSpec(memory_space=pltpu.SMEM)] + [vmem] * (2 + len(blocks)),
        out_specs=(vmem, vmem),
        scratch_shapes=[
            pltpu.VMEM((128, samples), jnp.float32),
            *[pltpu.VMEM((samples, samples), jnp.bfloat16)] * 3,
            pltpu.VMEM((late, features), jnp.bfloat16),
            pltpu.VMEM((samples, samples), jnp.float32),
        ],
        compiler_params=pltpu.CompilerParams(vmem_limit_bytes=KERNEL_VMEM),
    )(place, rows, gram, *blocks)


def on_device(inputs, out_grads, token_ids, in_signs, out_signs):
    local_count, length = token_ids.shape
    keep_mask = (token_ids >= RESERVED).astype(jnp.float32).reshape(-1, 1)
    in_proj = (project(inputs, in_signs) * keep_mask).reshape(local_count, length, -1)
    out_proj = project(out_grads, out_signs).reshape(local_count, length, -1)
    outer = jnp.einsum("sti,stj->sij", in_proj, out_proj, precision=lax.Precision.HIGHEST)
    per_sample = outer.reshape(local_count, -1).astype(jnp.bfloat16)
    first, pieces, exchange = gather_samples(per_sample, "dp")
    rows, gram, *pieces[-2:] = lax.optimization_barrier((*early(first), *pieces[-2:]))
    last = exchange(jnp.concatenate(pieces, axis=0))
    own_rows = per_sample.shape[1] // lax.axis_size("dp")
    place = lax.axis_index("dp").astype(jnp.int32).reshape(1)
    return tail(place, rows, gram, last, local_count, own_rows)


def solution(mesh):
    in_specs = (
        P(("groups", "dp"), None, None),
        P(("groups", "dp"), None, None),
        P(("groups", "dp"), None),
        P(),
        P(),
    )
    out_specs = (P(("groups", "dp"), None), P(("groups", "dp"), None))
    return jax.shard_map(
        on_device, mesh=mesh, in_specs=in_specs, out_specs=out_specs, check_vma=False
    )
```
